32 devices in a mesh: seq: 4 (over x, core), tensor: 8 (over z, y).
Axes of the slice: x: 2, y: 2, z: 4, core: 2. Of those that a mesh axis runs over, the one named last changes fastest.
Arguments:
- tokens: bfloat16 [2, 4096, 4096], P(None, 'seq', 'tensor'), may hold values from -6 to 6
- w_qkv: bfloat16 [4096, 3, 4096], P(None, None, 'tensor'), may hold values from -1 to 1
- q_gain: float32 [4096], P('tensor'), may hold values from 0.5 to 2.5
- k_gain: float32 [4096], P('tensor'), may hold values from 0.5 to 2.5
- w_out: bfloat16 [4096, 4096], P('tensor'), may hold values from -0.125 to 0.125
Outputs:
- mixed: bfloat16 [2, 4096, 4096], P(None, 'seq', 'tensor')
- peak: float32 [32], P('tensor')
- qk_scale: float32 [2, 2, 4096], P(None, None, 'seq')
The draws below stay inside these ranges and needn't reach their ends.
All inputs are finite; a program needn't handle non-finite values.
Results may differ from the reference program's by a relative error of at most 0.024.
Values may be sent and summed in bfloat16 or wider, within the bound.
A program may use at most 128 MiB of HBM per device.

```python
import math
import jax
import jax.numpy as jnp
from jax import lax

D = 4096
HEADS = 32
HEAD = 128
SEQS = 2
LENGTH = 4096
N_TENSOR = 8


def draw_tokens(key, part):
    base = jax.random.fold_in(key, 11)
    return jnp.clip(jax.random.normal(base, (SEQS, LENGTH, D), jnp.float32), -6.0, 6.0).astype(jnp.bfloat16)


def draw_w_qkv(key, part):
    base = jax.random.fold_in(key, 21)
    raw = jnp.clip(jax.random.normal(base, (D, 3, HEADS, HEAD), jnp.float32), -6.0, 6.0) / jnp.sqrt(jnp.float32(D))
    ramp = 0.6 * 3.0 ** (jnp.arange(HEADS, dtype=jnp.float32) / (HEADS - 1))
    scales = ramp * jnp.exp(jax.random.uniform(jax.random.fold_in(key, 22), (HEADS,), jnp.float32, jnp.log(0.8), jnp.log(1.25)))
    factors = jnp.stack([scales, scales, jnp.ones((HEADS,), jnp.float32)])
    raw = raw * factors[None, :, :, None]
    return jnp.clip(raw, -1.0, 1.0).reshape(D, 3, D).astype(jnp.bfloat16)


def with_spikes(values, own_key, source, target, shards_of, factor):
    def block_of(dim):
        return (jnp.arange(values.shape[dim]) // (values.shape[dim] // shards_of)).reshape((-1,) + (1,) * (values.ndim - 1 - dim))

    one_side = jax.random.permutation(own_key, shards_of)[block_of(target)]
    far = (block_of(target) + shards_of // 2) % shards_of
    return jnp.where((block_of(source) == one_side) | (block_of(source) == far), factor * values, values)


def block_levels(stream_key, extent, split, low, high):
    def one(axis_at, shards_of):
        steps = jax.random.uniform(jax.random.fold_in(jax.random.fold_in(stream_key, 6), axis_at), (shards_of,), jnp.float32, low / len(split), high / len(split))
        return jnp.repeat(jnp.exp(steps), extent[axis_at] // shards_of).reshape((-1,) + (1,) * (len(extent) - axis_at - 1))

    loudness = one(*split[0])
    for cut in split[1:]:
        loudness = loudness * one(*cut)
    return loudness


def gaussian_with(own_key, shape, scale, bound, cuts, heavy, kind=jnp.bfloat16):
    array = scale * jax.random.normal(own_key, shape, jnp.float32)
    if cuts:
        array = array * block_levels(own_key, shape, cuts, -0.22, 0.18)
    return jnp.clip(with_spikes(array, jax.random.fold_in(own_key, 3), *heavy), -bound, bound).astype(kind)


def setup_inputs(seed: int = 0) -> dict:
    splits = jax.random.split(jax.random.key(seed), 6)
    return {
        "tokens": draw_tokens(jax.random.fold_in(splits[5], 71), 0),
        "w_qkv": draw_w_qkv(jax.random.fold_in(splits[5], 71), 0),
        "q_gain": jnp.clip(jnp.exp(math.log(2.5) - 1.609438 * jax.random.uniform(splits[2], (D,), jnp.float32) ** block_levels(splits[2], (D,), ((0, 8),), -0.2, 0.2)), 0.5, 2.5),
        "k_gain": jnp.clip(jnp.exp(math.log(2.5) - 1.609438 * jax.random.uniform(splits[3], (D,), jnp.float32) ** block_levels(splits[3], (D,), ((0, 8),), -0.2, 0.2)), 0.5, 2.5),
        "w_out": gaussian_with(splits[4], (D, D), D ** -0.5, 0.125, ((0, 8),), (0, 1, 8, 2.0)),
    }


EPS = 1e-06
ROPE_BASE = 500000.0
NEG = -1e+30

def rope_tables(positions):
    half = HEAD // 2
    freq = ROPE_BASE ** (-(jnp.arange(half, dtype=jnp.float32) * 2.0) / HEAD)
    angle = positions[:, None] * freq[None, :]
    return (jnp.cos(angle), jnp.sin(angle))

def rotate(values, cosine, sine):
    half = values.shape[-1] // 2
    first = values[..., :half]
    second = values[..., half:]
    cosine = cosine[:, None, :]
    sine = sine[:, None, :]
    return jnp.concatenate([first * cosine - second * sine, second * cosine + first * sine], -1)

def reference(tokens, w_qkv, q_gain, k_gain, w_out):
    flat = tokens.reshape(SEQS * LENGTH, D)
    query = jnp.dot(flat, w_qkv[:, 0, :], preferred_element_type=jnp.float32)
    keyed = jnp.dot(flat, w_qkv[:, 1, :], preferred_element_type=jnp.float32)
    value = jnp.dot(flat, w_qkv[:, 2, :], preferred_element_type=jnp.float32)
    inv_query = lax.rsqrt(lax.optimization_barrier(jnp.mean(query * query, -1)) + EPS)
    inv_key = lax.rsqrt(lax.optimization_barrier(jnp.mean(keyed * keyed, -1)) + EPS)
    positions = jnp.arange(LENGTH, dtype=jnp.float32)
    cosine, sine = rope_tables(positions)
    q_norm = (query * inv_query[:, None] * q_gain[None, :]).reshape(SEQS, LENGTH, HEADS, HEAD)
    k_norm = (keyed * inv_key[:, None] * k_gain[None, :]).reshape(SEQS, LENGTH, HEADS, HEAD)
    q_rot = lax.optimization_barrier(rotate(q_norm, cosine, sine).astype(jnp.bfloat16))
    k_rot = lax.optimization_barrier(rotate(k_norm, cosine, sine).astype(jnp.bfloat16))
    v_b = lax.optimization_barrier(value.astype(jnp.bfloat16)).reshape(SEQS, LENGTH, HEADS, HEAD)
    q_heads = q_rot.transpose(2, 0, 1, 3)
    k_heads = k_rot.transpose(2, 0, 1, 3)
    v_heads = v_b.transpose(2, 0, 1, 3)
    causal = jnp.arange(LENGTH)[None, :] <= jnp.arange(LENGTH)[:, None]
    scale = HEAD ** (-0.5)

    def attend(operands):
        qh, kh, vh = operands
        scores = jnp.einsum('sqd,skd->sqk', qh.astype(jnp.float32), kh.astype(jnp.float32)) * scale
        scores = jnp.where(causal[None], scores, NEG)
        top = lax.optimization_barrier(jnp.max(scores, -1))
        weights = jnp.where(causal[None], jnp.exp(scores - top[..., None]), 0.0)
        denom = lax.optimization_barrier(jnp.sum(weights, -1))
        rounded = lax.optimization_barrier(weights.astype(jnp.bfloat16)).astype(jnp.float32)
        mixed = jnp.einsum('sqk,skd->sqd', rounded, vh.astype(jnp.float32))
        return ((mixed / denom[..., None]).astype(jnp.bfloat16), jnp.max(top))
    outputs, peak = lax.map(attend, (q_heads, k_heads, v_heads))
    attended = lax.optimization_barrier(outputs.transpose(1, 2, 0, 3).reshape(SEQS * LENGTH, D))
    group = D // N_TENSOR

    def add_group(total, index):
        cols = lax.dynamic_slice_in_dim(attended, index * group, group, 1)
        rows = lax.dynamic_slice_in_dim(w_out, index * group, group, 0)
        term = lax.optimization_barrier(jnp.dot(cols, rows, preferred_element_type=jnp.float32).astype(jnp.bfloat16))
        return (total + term.astype(jnp.float32), None)
    total, unused = lax.scan(add_group, jnp.zeros((SEQS * LENGTH, D), jnp.float32), jnp.arange(N_TENSOR, dtype=jnp.int32))
    mixed = total.astype(jnp.bfloat16).reshape(SEQS, LENGTH, D)
    qk_scale = jnp.stack([inv_query, inv_key]).reshape(2, SEQS, LENGTH)
    return (mixed, peak, qk_scale)
```

```python
import functools

import jax
import jax.numpy as jnp
from jax import lax
from jax.experimental import pallas as pl
from jax.experimental.pallas import tpu as pltpu
from jax.sharding import PartitionSpec as P

HEADS = 32
EPS = 1e-06
ROPE_BASE = 500000.0
NEG = -1e30
LOG2E = 1.4426950408889634
BLOCK_Q = 512
BLOCK_K = 1024


def rope_tables(positions, head):
    half = head // 2
    freq = ROPE_BASE ** (-(jnp.arange(half, dtype=jnp.float32) * 2.0) / head)
    angle = positions[:, None] * freq[None, :]
    cosine, sine = jnp.cos(angle), jnp.sin(angle)
    return (
        jnp.concatenate([cosine, cosine], -1),
        jnp.concatenate([-sine, sine], -1),
    )


def flash_kernel(use_ref, q_ref, *refs, blocks, bq, bk):
    k_refs, v_refs = refs[:blocks], refs[blocks : 2 * blocks]
    o_ref, top_ref, m_s, l_s, acc_s = refs[2 * blocks :]
    rows = q_ref.shape[0]
    best = jnp.full((1, 128), NEG, jnp.float32)
    for i in range(rows // bq):
        q = q_ref[pl.ds(i * bq, bq), :]
        m_s[...] = jnp.full(m_s.shape, NEG, jnp.float32)
        l_s[...] = jnp.zeros(l_s.shape, jnp.float32)
        acc_s[...] = jnp.zeros(acc_s.shape, jnp.float32)

        def step(k, v, masked):
            s = lax.dot_general(q, k, (((1,), (1,)), ((), ())), preferred_element_type=jnp.float32)
            if masked:
                row = lax.broadcasted_iota(jnp.int32, s.shape, 0)
                col = lax.broadcasted_iota(jnp.int32, s.shape, 1)
                s = jnp.where(col <= row, s, NEG)
            m_old = m_s[...]
            m_new = jnp.maximum(m_old, jnp.max(s, -1, keepdims=True))
            p = jnp.exp2(s - jnp.tile(m_new, (1, s.shape[1] // 128)))
            alpha = jnp.exp2(m_old - m_new)
            part = p[:, :128]
            for j in range(1, s.shape[1] // 128):
                part = part + p[:, j * 128 : (j + 1) * 128]
            l_s[...] = l_s[...] * alpha + part
            acc_s[...] = acc_s[...] * alpha + jnp.dot(
                p.astype(jnp.bfloat16), v, preferred_element_type=jnp.float32
            )
            m_s[...] = m_new

        step(k_refs[0][pl.ds(i * bq, bq), :], v_refs[0][pl.ds(i * bq, bq), :], True)
        for j in range(i):
            step(k_refs[0][pl.ds(j * bq, bq), :], v_refs[0][pl.ds(j * bq, bq), :], False)
        for e in range(1, blocks):

            @pl.when(use_ref[e] > 0)
            def _():
                for j in range(rows // bk):
                    step(k_refs[e][pl.ds(j * bk, bk), :], v_refs[e][pl.ds(j * bk, bk), :], False)

        denom = jnp.sum(l_s[...], -1, keepdims=True)
        o_ref[pl.ds(i * bq, bq), :] = (acc_s[...] / denom).astype(o_ref.dtype)
        best = jnp.maximum(best, jnp.max(m_s[...], 0, keepdims=True))
    top_ref[...] = jnp.broadcast_to(best, top_ref.shape)


def flash(q, keys, values, use, head):
    rows, dloc = q.shape
    heads = dloc // head
    blocks = len(keys)
    bq = min(BLOCK_Q, rows)
    bk = min(BLOCK_K, rows)
    spec = pl.BlockSpec((rows, head), lambda h, f: (0, h))
    return pl.pallas_call(
        functools.partial(flash_kernel, blocks=blocks, bq=bq, bk=bk),
        grid_spec=pltpu.PrefetchScalarGridSpec(
            num_scalar_prefetch=1,
            grid=(heads,),
            in_specs=[spec] * (1 + 2 * blocks),
            out_specs=[spec, pl.BlockSpec((None, 8, 128), lambda h, f: (h, 0, 0))],
            scratch_shapes=[
                pltpu.VMEM((bq, 128), jnp.float32),
                pltpu.VMEM((bq, 128), jnp.float32),
                pltpu.VMEM((bq, head), jnp.float32),
            ],
        ),
        out_shape=[
            jax.ShapeDtypeStruct((rows, dloc), jnp.bfloat16),
            jax.ShapeDtypeStruct((heads, 8, 128), jnp.float32),
        ],
        compiler_params=pltpu.CompilerParams(
            dimension_semantics=("arbitrary",), vmem_limit_bytes=32 * 1024 * 1024
        ),
        cost_estimate=pl.CostEstimate(
            flops=8 * rows * rows * blocks * dloc,
            bytes_accessed=4 * rows * blocks * dloc,
            transcendentals=0,
        ),
    )(use, q, *keys, *values)


def earlier_blocks(block, count, across):
    outer = [
        lax.ppermute(block, "seq", [(i, i + across * d) for i in range(count - across * d)])
        for d in range(1, count // across)
    ]
    swap = [(i, i + 1 - 2 * (i % 2)) for i in range(count)]
    near = lax.ppermute(block, "seq", swap)
    return [block, near] + outer + [lax.ppermute(got, "seq", swap) for got in outer]


def shards(tokens, w_qkv, q_gain, k_gain, w_out):
    seqs, tok, dloc = tokens.shape
    width = w_qkv.shape[0]
    head = width // HEADS
    heads_here = dloc // head
    flat_w = w_qkv.reshape(width, 3 * dloc)
    own_index = lax.axis_index("seq")
    q_index = own_index * tok + jnp.arange(tok, dtype=jnp.int32)
    cosine, sine = rope_tables(q_index.astype(jnp.float32), head)
    count = lax.axis_size("seq")
    chip = own_index // 2
    outer_flags = [(chip >= d).astype(jnp.int32) for d in range(1, count // 2)]
    use = jnp.stack([jnp.int32(1), (own_index % 2).astype(jnp.int32)] + outer_flags + outer_flags)
    scale = head ** (-0.5)

    def prepare(projection, scale_row, gain):
        normed = (projection * scale_row[:, None] * gain[None, :]).reshape(tok, heads_here, head)
        swapped = jnp.roll(normed, head // 2, axis=-1)
        turned = normed * cosine[:, None, :] + swapped * sine[:, None, :]
        return turned.astype(jnp.bfloat16).reshape(tok, dloc)

    gathered = [lax.all_gather(tokens[s], "tensor", axis=1, tiled=True) for s in range(seqs)]
    mixed, tops, inverses = [], [], []
    for s in range(seqs):
        whole = gathered[s]
        if s > 0:
            whole, partial_out = lax.optimization_barrier((whole, partial_out))
            mixed.append(lax.psum_scatter(partial_out, "tensor", scatter_dimension=1, tiled=True))
        paired = jnp.dot(whole, flat_w[:, : 2 * dloc], preferred_element_type=jnp.float32)
        query, keyed = paired[:, :dloc], paired[:, dloc:]
        squares = jnp.stack([jnp.sum(query * query, 1), jnp.sum(keyed * keyed, 1)])
        totals = lax.psum(squares, "tensor")
        inverse = lax.rsqrt(totals / width + EPS)
        inverses.append(inverse)
        value = jnp.dot(whole, flat_w[:, 2 * dloc :], preferred_element_type=jnp.float32)
        q_ready = prepare(query, inverse[0], q_gain * (scale * LOG2E))
        k_ready = prepare(keyed, inverse[1], k_gain)
        keys = earlier_blocks(k_ready, count, 2)
        values = earlier_blocks(value.astype(jnp.bfloat16), count, 2)
        attended, top = flash(q_ready, keys, values, use, head)
        tops.append(jnp.max(top, axis=(1, 2)))
        partial_out = jnp.dot(attended, w_out, preferred_element_type=jnp.float32).astype(
            jnp.bfloat16
        )
    mixed.append(lax.psum_scatter(partial_out, "tensor", scatter_dimension=1, tiled=True))
    peak = lax.pmax(functools.reduce(jnp.maximum, tops), "seq") * (1.0 / LOG2E)
    return (jnp.stack(mixed), peak, jnp.stack(inverses, 1))


def solution(mesh):
    return jax.shard_map(
        shards,
        mesh=mesh,
        in_specs=(
            P(None, "seq", "tensor"),
            P(None, None, "tensor"),
            P("tensor"),
            P("tensor"),
            P("tensor", None),
        ),
        out_specs=(P(None, "seq", "tensor"), P("tensor"), P(None, None, "seq")),
        check_vma=False,
    )
```
